32 devices in a mesh: site: 2 (over y), pts: 16 (over z, x, core).
Axes of the slice: x: 2, y: 2, z: 4, core: 2. Of those that a mesh axis runs over, the one named last changes fastest.
Arguments:
- green_tensors: bfloat16 [512, 4, 6, 2, 1024], P(('site', 'pts')), parts along dimension 0, may hold values from -6 to 6
- block_lists: int32 [32, 32], P(('site', 'pts')), parts along dimension 0, may hold values from 0 to 255, as said below
- block_count: int32 [32], P(('site', 'pts')), parts along dimension 0, may hold values from 1 to 32
- onset_steps: int32 [32, 16, 128], P(('site', 'pts')), parts along dimension 0, may hold values from 0 to 255
- slip_amount: float32 [32, 16, 128], P(('site', 'pts')), parts along dimension 0, may hold values from 0.2 to 2
- mechanism: float32 [32, 6], P(('site', 'pts')), parts along dimension 0, may hold values from -2.4 to 2.4
- slip_rate: float32 [32, 16, 128], P(('site', 'pts')), parts along dimension 0, may hold values from 0.005 to 0.05
Outputs:
- seismograms: float32 [32, 16, 2, 1024], P(('site', 'pts')), parts along dimension 0
The draws below stay inside these ranges and needn't reach their ends.
There are 2 independent parts, one for each index of `site`. The reference program is written for one: setup_inputs(seed, part) draws one part's arguments, and reference() takes and returns one part's arrays. A program takes and returns all parts, laid end to end along the dimension named above; each array names one. Nothing has to cross between parts.
Inputs may be any that keep to these rules, and one draw needn't show every extreme that they name: `block_lists`: numbers of point blocks; the ruptures held by one device name at most 2 entries in blocks held by any one device, and exactly 2 for some holder.
All inputs are finite; a program needn't handle non-finite values.
Results may differ from the reference program's by a relative error of at most 0.0003.
Values may be sent and summed in bfloat16 or wider, within the bound.
No kernel may reach another device: no remote copies, remote signals or barrier semaphores. Data moves between devices by JAX's collectives and lax.ppermute only.
A program may use at most 128 MiB of HBM per device.

```python
import math
import jax
import jax.numpy as jnp
from jax import lax

NT = 1024
P_SIZE = 4
K = 32
V = 16
L = 128
MAXON = 256
BD = 16
RD = 1
NB = 256
R = 16
N_PTS = 16


def draw_block_lists(key, part):
    entries = RD * K

    def per_worker(worker):
        worker_key = jax.random.fold_in(jax.random.fold_in(key, 11), worker)
        holders = jax.random.permutation(worker_key, N_PTS)
        order = jnp.arange(entries, dtype=jnp.int32)
        holder_of = holders[order % N_PTS]
        local_block = jax.random.randint(jax.random.fold_in(worker_key, 1), (entries,), 0, BD)
        return (holder_of * BD + local_block).astype(jnp.int32)
    lists = jax.vmap(per_worker)(jnp.arange(N_PTS, dtype=jnp.int32))
    return lists.reshape(RD * N_PTS, K)


def set_ends(values, own_key, low, top_value):
    index_at = [jax.random.randint(jax.random.fold_in(own_key, axis), (), 0, length) for axis, length in enumerate(values.shape)]
    main_axis = values.shape.index(max(values.shape))
    beside = index_at[:main_axis] + [(index_at[main_axis] + 1) % values.shape[main_axis]] + index_at[main_axis + 1:]
    return values.at[tuple(index_at)].set(low).at[tuple(beside)].set(top_value)


def steps_of(own_key, dims, cuts, smallest, top_value):
    def one(dim, blocks):
        draws = jax.random.uniform(jax.random.fold_in(jax.random.fold_in(own_key, 6), dim), (blocks,), jnp.float32, smallest / len(cuts), top_value / len(cuts))
        return jnp.repeat(jnp.exp(draws), dims[dim] // blocks).reshape((-1,) + (1,) * (len(dims) - dim - 1))

    gain = one(*cuts[0])
    for cut in cuts[1:]:
        gain = gain * one(*cut)
    return gain


def normal_values(rng, shape, scale, limit, cuts=(), kind=jnp.bfloat16):
    array = scale * jax.random.normal(rng, shape, jnp.float32)
    if cuts:
        array = array * steps_of(rng, shape, cuts, -0.22, 0.18)
    return jnp.clip(array, -limit, limit).astype(kind)


def setup_inputs(seed: int = 0, part: int = 0) -> dict:
    keys = jax.random.split(jax.random.key(seed), 8)
    part_keys = jax.random.split(jax.random.fold_in(keys[7], part), 8)
    return {
        "green_tensors": normal_values(part_keys[0], (NB, P_SIZE, 6, 2, NT), 1.0, 6.0, ((0, 16),)),
        "block_lists": draw_block_lists(jax.random.fold_in(jax.random.fold_in(keys[7], part), 71), part),
        "block_count": set_ends(jax.random.randint(part_keys[2], (R,), 1, K + 1), jax.random.fold_in(part_keys[2], 1), 1, K).astype(jnp.int32),
        "onset_steps": set_ends(jax.random.randint(part_keys[3], (R, V, K * P_SIZE), 0, MAXON), jax.random.fold_in(part_keys[3], 1), 0, MAXON - 1).astype(jnp.int32),
        "slip_amount": jnp.clip(jnp.exp(math.log(2.0) - 2.3025851 * jax.random.uniform(part_keys[4], (R, V, K * P_SIZE), jnp.float32) ** steps_of(part_keys[4], (R, V, K * P_SIZE), ((0, 16),), -0.2, 0.2)), 0.2, 2.0),
        "mechanism": normal_values(part_keys[5], (R, 6), 0.4, 2.4, ((0, 16),), jnp.float32),
        "slip_rate": jnp.clip(jnp.exp(math.log(0.05) - 2.3025851 * jax.random.uniform(part_keys[6], (R, V, L), jnp.float32) ** steps_of(part_keys[6], (R, V, L), ((0, 16),), -0.2, 0.2)), 0.005, 0.05),
    }


def lag_traces(traces, onsets):
    steps = jnp.arange(traces.shape[-1], dtype=jnp.int32)
    source = steps[None, :] - onsets[:, None]
    inside = source >= 0
    picked = jnp.take_along_axis(traces, jnp.broadcast_to(jnp.maximum(source, 0)[:, None, :], traces.shape), axis=2)
    return jnp.where(inside[:, None, :], picked, 0.0)


def weighted_sum(traces, weights, onsets):
    def per_variation(weight_row, onset_row):
        return jnp.sum(weight_row[:, None, None] * lag_traces(traces, onset_row), axis=0)
    return jax.vmap(per_variation)(weights, onsets)


def reference(green_tensors, block_lists, block_count, onset_steps, slip_amount, mechanism, slip_rate):
    listed = block_lists.shape[1]
    length = green_tensors.shape[-1]

    def per_rupture(inputs):
        blocks, listed_count, onset_rows, slip_rows, mech_row, rate_rows = inputs
        chosen = jnp.take(green_tensors, blocks, axis=0).astype(jnp.float32)
        traces = jnp.einsum("kpsct,s->kpct", chosen, mech_row, precision=lax.Precision.HIGHEST)
        kept_mask = (jnp.arange(listed, dtype=jnp.int32) < listed_count).astype(jnp.float32)
        points = chosen.shape[1]
        weights = slip_rows * jnp.repeat(kept_mask, points)[None, :]
        motion = weighted_sum(traces.reshape(-1, 2, length), weights, onset_rows)

        def convolve_row(signal, kernel):
            return jnp.convolve(signal, kernel, precision=lax.Precision.HIGHEST)[:length]

        return jax.vmap(jax.vmap(convolve_row, (0, None)), (0, 0))(motion, rate_rows)

    return lax.map(per_rupture, (block_lists, block_count, onset_steps, slip_amount, mechanism, slip_rate))
```

```python
import functools

import jax
import jax.numpy as jnp
from jax import lax
from jax.experimental import pallas as pl
from jax.experimental.pallas import tpu as pltpu
from jax.sharding import PartitionSpec as P

MAXON = 256
FINE = 8
LANES = 128
F32 = jnp.float32
BF16 = jnp.bfloat16


def split(x):
    hi = x.astype(BF16)
    return hi, (x - hi.astype(F32)).astype(BF16)


def dot3(a_hi, a_lo, b_hi, b_lo):
    dot = functools.partial(jnp.dot, preferred_element_type=F32)
    return dot(a_hi, b_hi) + (dot(a_hi, b_lo) + dot(a_lo, b_hi))


def contract_kernel(block_ref, mech_ref, tensors_ref, out_ref, *, slots, points, strains):
    def one_slot(i, carry):
        block = block_ref[i]
        source = i // slots
        factors = [mech_ref[source, s] for s in range(strains)]
        for p in range(points):
            total = factors[0] * tensors_ref[block, p, 0].astype(F32)
            for s in range(1, strains):
                total = total + factors[s] * tensors_ref[block, p, s].astype(F32)
            out_ref[i, p] = total
        return carry

    lax.fori_loop(0, out_ref.shape[0], one_slot, 0, unroll=2)


def prepare_kernel(onset_ref, weight_ref, rate_ref, a_hi_ref, a_lo_ref, t_hi_ref, t_lo_ref):
    variations, points = onset_ref.shape
    taps = rate_ref.shape[1]
    onsets = onset_ref[...]
    weights = weight_ref[...]
    w_hi = weights.astype(BF16).astype(F32)
    w_lo = weights - w_hi
    for coarse in range(MAXON // FINE):
        for fine in range(FINE):
            hit = onsets == coarse * FINE + fine
            rows = pl.ds(coarse * variations, variations)
            cols = pl.ds(fine * points, points)
            a_hi_ref[rows, cols] = jnp.where(hit, w_hi, 0.0).astype(BF16)
            a_lo_ref[rows, cols] = jnp.where(hit, w_lo, 0.0).astype(BF16)
    row = lax.broadcasted_iota(jnp.int32, (taps, taps), 0)
    col = lax.broadcasted_iota(jnp.int32, (taps, taps), 1)
    for v in range(variations):
        rates = jnp.broadcast_to(rate_ref[pl.ds(v, 1), :], (taps, taps))
        turned = pltpu.roll(rates, 0, 1, stride=1, stride_axis=0)
        hi, lo = split(jnp.where(col >= row, turned, 0.0))
        t_hi_ref[v, pl.ds(0, taps), :] = hi
        t_lo_ref[v, pl.ds(0, taps), :] = lo
        hi, lo = split(jnp.where(col < row, turned, 0.0))
        t_hi_ref[v, pl.ds(taps, taps), :] = hi
        t_lo_ref[v, pl.ds(taps, taps), :] = lo


def synth_kernel(row_ref, got_ref, a_hi_ref, a_lo_ref, t_hi_ref, t_lo_ref, out_ref,
                 base_ref, x_hi_ref, x_lo_ref, acc_ref, motion_ref, *, listed, points):
    variations, rows = out_ref.shape[:2]
    q = listed * points
    comps = 2
    blocks = rows // comps

    def place(k, carry):
        source = row_ref[k]
        for p in range(points):
            base_ref[pl.ds(pl.multiple_of((k * points + p) * rows, rows), rows), :] = got_ref[source, p]
        return carry

    lax.fori_loop(0, listed, place, 0, unroll=4)
    lane = lax.broadcasted_iota(jnp.int32, (q, LANES), 1)
    for c in range(comps):
        before = [jnp.zeros((q, LANES), F32)] * FINE
        for block in range(blocks):
            r = block * comps + c
            here = base_ref[pl.ds(r, q, stride=rows), :]
            at = pl.ds((c * blocks + block) * LANES, LANES)
            for fine in range(FINE):
                turned = pltpu.roll(here, fine, 1) if fine else here
                value = jnp.where(lane >= fine, turned, before[fine]) if fine else here
                hi, lo = split(value)
                x_hi_ref[pl.ds(fine * q, q), at] = hi
                x_lo_ref[pl.ds(fine * q, q), at] = lo
                before[fine] = turned
    acc_ref[...] = dot3(a_hi_ref[...], a_lo_ref[...], x_hi_ref[...], x_lo_ref[...])
    lane = lax.broadcasted_iota(jnp.int32, (variations, LANES), 1)
    zero = jnp.zeros((variations, LANES), F32)
    half = LANES // FINE
    far_count = MAXON // LANES
    pad = motion_ref.shape[0] // variations
    motion_ref[...] = jnp.zeros(motion_ref.shape, F32)
    for c in range(comps):
        before = [zero] * half
        for block in range(blocks):
            total = zero
            for coarse in range(half):
                value = zero
                for far in range(far_count):
                    if block - far < 0:
                        continue
                    at = pl.ds((c * blocks + block - far) * LANES, LANES)
                    value = value + acc_ref[pl.ds((far * half + coarse) * variations, variations), at]
                turned = pltpu.roll(value, coarse * FINE, 1) if coarse else value
                total = total + (jnp.where(lane >= coarse * FINE, turned, before[coarse]) if coarse else turned)
                before[coarse] = turned
            motion_ref[pl.ds(FINE + block * comps + c, variations, stride=pad), :] = total
    for v in range(variations):
        here = motion_ref[pl.ds(v * pad + FINE, rows), :]
        earlier = motion_ref[pl.ds(v * pad + FINE - comps, rows), :]
        h_hi, h_lo = split(jnp.concatenate([here, earlier], axis=1))
        out_ref[v] = dot3(h_hi, h_lo, t_hi_ref[v], t_lo_ref[v])


VMEM = pl.BlockSpec(memory_space=pltpu.VMEM)
SMEM = pl.BlockSpec(memory_space=pltpu.SMEM)


def local(green_tensors, block_lists, block_count, onset_steps, slip_amount, mechanism, slip_rate):
    held, points, strains, comps, length = green_tensors.shape
    ruptures, listed = block_lists.shape
    variations = onset_steps.shape[1]
    taps = slip_rate.shape[-1]
    devices = lax.axis_size("pts")
    capacity = max(1, ruptures * listed // devices)
    blocks = length // LANES
    rows = blocks * comps
    q = listed * points

    tensors = green_tensors.reshape(held, points, strains, comps, blocks, LANES)
    tensors = tensors.transpose(0, 1, 2, 4, 3, 5).reshape(held, points, strains, rows, LANES)

    entries = block_lists.reshape(ruptures * listed)
    holder = entries // held
    order = jnp.arange(ruptures * listed, dtype=jnp.int32)
    same = (holder[:, None] == holder[None, :]) & (order[None, :] < order[:, None])
    rank = jnp.sum(same.astype(jnp.int32), axis=1)
    slot_of = holder * capacity + rank
    slot_ids = jnp.arange(devices * capacity, dtype=jnp.int32)
    wanted = jnp.sum(
        jnp.where(slot_of[None, :] == slot_ids[:, None], (entries % held)[None, :], 0), axis=1
    )
    request = jnp.concatenate(
        [
            wanted.astype(F32).reshape(devices, capacity),
            jnp.broadcast_to(mechanism.reshape(1, strains), (devices, strains)),
        ],
        axis=1,
    )
    asked = lax.all_to_all(request, "pts", split_axis=0, concat_axis=0, tiled=True)
    block_of = asked[:, :capacity].astype(jnp.int32).reshape(devices * capacity)
    factors = asked[:, capacity:]

    kept = (jnp.arange(q, dtype=jnp.int32) // points) < block_count[0]
    weights = jnp.where(kept[None, :], slip_amount[0], 0.0)
    coarse_rows = MAXON // FINE * variations
    prepared = pl.pallas_call(
        prepare_kernel,
        name="prepare",
        out_shape=(
            jax.ShapeDtypeStruct((coarse_rows, FINE * q), BF16),
            jax.ShapeDtypeStruct((coarse_rows, FINE * q), BF16),
            jax.ShapeDtypeStruct((variations, 2 * taps, taps), BF16),
            jax.ShapeDtypeStruct((variations, 2 * taps, taps), BF16),
        ),
        in_specs=[VMEM, VMEM, VMEM],
        out_specs=(VMEM, VMEM, VMEM, VMEM),
    )(onset_steps[0], weights, slip_rate[0])

    outgoing = pl.pallas_call(
        functools.partial(contract_kernel, slots=capacity, points=points, strains=strains),
        name="contract",
        out_shape=jax.ShapeDtypeStruct((devices * capacity, points, rows, LANES), F32),
        in_specs=[SMEM, SMEM, VMEM],
        out_specs=VMEM,
    )(block_of, factors, tensors)
    incoming = lax.all_to_all(outgoing, "pts", split_axis=0, concat_axis=0, tiled=True)

    result = pl.pallas_call(
        functools.partial(synth_kernel, listed=listed, points=points),
        name="synthesize",
        out_shape=jax.ShapeDtypeStruct((variations, rows, LANES), F32),
        in_specs=[SMEM, VMEM, VMEM, VMEM, VMEM, VMEM],
        out_specs=VMEM,
        scratch_shapes=[
            pltpu.VMEM((q * rows, LANES), F32),
            pltpu.VMEM((FINE * q, rows * LANES), BF16),
            pltpu.VMEM((FINE * q, rows * LANES), BF16),
            pltpu.VMEM((coarse_rows, rows * LANES), F32),
            pltpu.VMEM((variations * (rows + FINE), LANES), F32),
        ],
    )(slot_of, incoming, *prepared)
    result = result.reshape(variations, blocks, comps, LANES).transpose(0, 2, 1, 3)
    return result.reshape(1, variations, comps, length)


def solution(mesh):
    in_specs = (
        P(("site", "pts"), None, None, None, None),
        P(("site", "pts"), None),
        P(("site", "pts")),
        P(("site", "pts"), None, None),
        P(("site", "pts"), None, None),
        P(("site", "pts"), None),
        P(("site", "pts"), None, None),
    )
    out_specs = P(("site", "pts"), None, None, None)
    return jax.shard_map(local, mesh=mesh, in_specs=in_specs, out_specs=out_specs, check_vma=False)
```

```python
import functools

import jax
import jax.numpy as jnp
from jax import lax
from jax.experimental import pallas as pl
from jax.experimental.pallas import tpu as pltpu
from jax.sharding import PartitionSpec as P

MAXON = 256
FINE = 8
LANES = 128
F32 = jnp.float32
BF16 = jnp.bfloat16


def split(x):
    hi = x.astype(BF16)
    return hi, (x - hi.astype(F32)).astype(BF16)


def dot(a, b):
    return jnp.dot(a, b, preferred_element_type=F32)


def request_kernel(lists_ref, mech_ref, request_ref, slot_ref, *, held, capacity):
    devices = request_ref.shape[0]
    listed = lists_ref.shape[1]
    entries = lists_ref[...].astype(F32)
    holder = jnp.floor((entries + 0.5) * (1.0 / held))
    inside = entries - holder * held
    row = lax.broadcasted_iota(jnp.int32, (listed, listed), 0)
    col = lax.broadcasted_iota(jnp.int32, (listed, listed), 1)
    across = jnp.broadcast_to(holder, (listed, listed))
    down = jnp.sum(jnp.where(row == col, across, 0.0), axis=1, keepdims=True)
    same = jnp.where((down == across) & (row < col), 1.0, 0.0)
    rank = jnp.sum(same, axis=0, keepdims=True)
    slot_ref[...] = (holder * capacity + rank).astype(jnp.int32)
    request_ref[:, capacity:] = jnp.broadcast_to(mech_ref[...], (devices, mech_ref.shape[1]))
    device = lax.broadcasted_iota(jnp.int32, (devices, listed), 0).astype(F32)
    for j in range(capacity):
        hit = (device == holder) & (rank == j)
        request_ref[:, j:j + 1] = jnp.sum(jnp.where(hit, inside, 0.0), axis=1, keepdims=True)


CODE_STEPS = 256.0
CODE_BIAS = 100.0
VALUE_TOP = 32767.0
CODE_ROWS = 8


def encode(x):
    top = jnp.max(jnp.max(jnp.abs(x), axis=0, keepdims=True), axis=1, keepdims=True)
    code = jnp.ceil((jnp.log2(jnp.maximum(top, 1e-30)) + CODE_BIAS) * CODE_STEPS)
    code = jnp.broadcast_to(code, (1, LANES))
    scale = jnp.exp2(15.0 - (code * (1.0 / CODE_STEPS) - CODE_BIAS))
    value = jnp.clip(jnp.floor(x * scale + 0.5), -VALUE_TOP, VALUE_TOP)
    return value.astype(jnp.int32).astype(jnp.int16), code


def decode(y, codes, entry):
    place = lax.broadcasted_iota(jnp.int32, codes.shape, 0)
    code = jnp.sum(jnp.where(place == entry, codes, 0.0), axis=0, keepdims=True)
    scale = jnp.exp2((code * (1.0 / CODE_STEPS) - CODE_BIAS) - 15.0)
    return y.astype(jnp.int32).astype(F32) * scale


def contract_kernel(asked_ref, tensors_ref, out_ref, *, slots, points, strains):
    rows = tensors_ref.shape[3]
    code_rows = out_ref.shape[1] - slots * points * rows

    def one_source(source, carry):
        factors = [asked_ref[source, slots + s] for s in range(strains)]
        place = lax.broadcasted_iota(jnp.int32, (code_rows, LANES), 0)
        codes = jnp.zeros((code_rows, LANES), F32)
        for j in range(slots):
            block = asked_ref[source, j].astype(jnp.int32)
            for p in range(points):
                total = factors[0] * tensors_ref[block, p, 0].astype(F32)
                for s in range(1, strains):
                    total = total + factors[s] * tensors_ref[block, p, s].astype(F32)
                entry = j * points + p
                value, code = encode(total)
                out_ref[source, pl.ds(entry * rows, rows), :] = value
                codes = jnp.where(place == entry, code, codes)
        out_ref[source, pl.ds(slots * points * rows, code_rows), :] = codes.astype(jnp.int32).astype(jnp.int16)
        return carry

    lax.fori_loop(0, out_ref.shape[0], one_source, 0, unroll=2)


def prepare_kernel(onset_ref, weight_ref, rate_ref, a_ref, t_hi_ref, t_lo_ref):
    variations, points = onset_ref.shape
    width = FINE * points
    taps = rate_ref.shape[1]
    onsets = onset_ref[...]
    weights = weight_ref[...]
    w_hi = weights.astype(BF16).astype(F32)
    w_lo = weights - w_hi
    for coarse in range(MAXON // FINE):
        for fine in range(FINE):
            hit = onsets == coarse * FINE + fine
            rows = pl.ds(coarse * variations, variations)
            near = jnp.where(hit, w_hi, 0.0).astype(BF16)
            a_ref[rows, pl.ds(fine * points, points)] = near
            a_ref[rows, pl.ds(width + fine * points, points)] = near
            a_ref[rows, pl.ds(2 * width + fine * points, points)] = jnp.where(hit, w_lo, 0.0).astype(BF16)
    row = lax.broadcasted_iota(jnp.int32, (taps, taps), 0)
    col = lax.broadcasted_iota(jnp.int32, (taps, taps), 1)
    for v in range(variations):
        rates = jnp.broadcast_to(rate_ref[pl.ds(v, 1), :], (taps, taps))
        turned = pltpu.roll(rates, 0, 1, stride=1, stride_axis=0)
        hi, lo = split(jnp.where(col >= row, turned, 0.0))
        t_hi_ref[v, pl.ds(0, taps), :] = hi
        t_lo_ref[v, pl.ds(0, taps), :] = lo
        hi, lo = split(jnp.where(col < row, turned, 0.0))
        t_hi_ref[v, pl.ds(taps, taps), :] = hi
        t_lo_ref[v, pl.ds(taps, taps), :] = lo


def synth_kernel(row_ref, got_ref, a_ref, t_hi_ref, t_lo_ref, out_ref,
                 base_ref, x_ref, acc_ref, motion_ref, *, listed, points, slots):
    variations, rows = out_ref.shape[:2]
    q = listed * points
    comps = 2
    blocks = rows // comps

    code_rows = got_ref.shape[1] - slots * points * rows

    def place(k, carry):
        slot = row_ref[0, k]
        source = slot // slots
        first = (slot % slots) * points
        codes = got_ref[source, pl.ds(slots * points * rows, code_rows), :].astype(jnp.int32).astype(F32)
        for p in range(points):
            value = got_ref[source, pl.ds(pl.multiple_of((first + p) * rows, rows), rows), :]
            base_ref[pl.ds(pl.multiple_of((k * points + p) * rows, rows), rows), :] = decode(value, codes, first + p)
        return carry

    lax.fori_loop(0, listed, place, 0, unroll=4)
    lane = lax.broadcasted_iota(jnp.int32, (q, LANES), 1)
    for c in range(comps):
        before = [jnp.zeros((q, LANES), F32)] * FINE
        for block in range(blocks):
            r = block * comps + c
            here = base_ref[pl.ds(r, q, stride=rows), :]
            at = pl.ds(block * LANES, LANES)
            for fine in range(FINE):
                turned = pltpu.roll(here, fine, 1) if fine else here
                value = jnp.where(lane >= fine, turned, before[fine]) if fine else here
                hi, lo = split(value)
                x_ref[c, pl.ds(fine * q, q), at] = hi
                x_ref[c, pl.ds((FINE + fine) * q, q), at] = lo
                before[fine] = turned
        both = 2 * FINE * q
        acc_ref[c] = dot(a_ref[:, :both], x_ref[c]) + dot(a_ref[:, both:], x_ref[c, :FINE * q])
    lane = lax.broadcasted_iota(jnp.int32, (variations, LANES), 1)
    zero = jnp.zeros((variations, LANES), F32)
    half = LANES // FINE
    far_count = MAXON // LANES
    pad = motion_ref.shape[0] // variations
    motion_ref[...] = jnp.zeros(motion_ref.shape, F32)
    for c in range(comps):
        before = [zero] * half
        for block in range(blocks):
            total = zero
            for coarse in range(half):
                value = zero
                for far in range(far_count):
                    if block - far < 0:
                        continue
                    at = pl.ds((block - far) * LANES, LANES)
                    value = value + acc_ref[c, pl.ds((far * half + coarse) * variations, variations), at]
                turned = pltpu.roll(value, coarse * FINE, 1) if coarse else value
                total = total + (jnp.where(lane >= coarse * FINE, turned, before[coarse]) if coarse else turned)
                before[coarse] = turned
            motion_ref[pl.ds(FINE + block * comps + c, variations, stride=pad), :] = total
    for v in range(variations):
        here = motion_ref[pl.ds(v * pad + FINE, rows), :]
        earlier = motion_ref[pl.ds(v * pad + FINE - comps, rows), :]
        h_hi, h_lo = split(jnp.concatenate([here, earlier], axis=1))
        out_ref[v] = dot(h_hi, t_hi_ref[v]) + (dot(h_lo, t_hi_ref[v]) + dot(h_hi, t_lo_ref[v]))


SMALL = pltpu.CompilerParams(vmem_limit_bytes=8 << 20)
LARGE = pltpu.CompilerParams(vmem_limit_bytes=20 << 20)
VMEM = pl.BlockSpec(memory_space=pltpu.VMEM)
SMEM = pl.BlockSpec(memory_space=pltpu.SMEM)


def local(green_tensors, block_lists, block_count, onset_steps, slip_amount, mechanism, slip_rate):
    held, points, strains, comps, length = green_tensors.shape
    ruptures, listed = block_lists.shape
    variations = onset_steps.shape[1]
    taps = slip_rate.shape[-1]
    devices = lax.axis_size("pts")
    capacity = max(1, ruptures * listed // devices)
    blocks = length // LANES
    rows = blocks * comps
    q = listed * points

    tensors = green_tensors.reshape(held, points, strains, comps, blocks, LANES)
    tensors = tensors.transpose(0, 1, 2, 4, 3, 5).reshape(held, points, strains, rows, LANES)

    request, slot_of = pl.pallas_call(
        functools.partial(request_kernel, held=held, capacity=capacity),
        name="request",
        out_shape=(
            jax.ShapeDtypeStruct((devices, capacity + strains), F32),
            jax.ShapeDtypeStruct((ruptures, listed), jnp.int32),
        ),
        compiler_params=SMALL,
    )(block_lists, mechanism)
    asked = lax.all_to_all(request, "pts", split_axis=0, concat_axis=0, tiled=True)

    kept = (jnp.arange(q, dtype=jnp.int32) // points) < block_count[0]
    weights = jnp.where(kept[None, :], slip_amount[0], 0.0)
    coarse_rows = MAXON // FINE * variations
    prepared = pl.pallas_call(
        prepare_kernel,
        name="prepare",
        out_shape=(
            jax.ShapeDtypeStruct((coarse_rows, 3 * FINE * q), BF16),
            jax.ShapeDtypeStruct((variations, 2 * taps, taps), BF16),
            jax.ShapeDtypeStruct((variations, 2 * taps, taps), BF16),
        ),
        in_specs=[VMEM, VMEM, VMEM],
        out_specs=(VMEM, VMEM, VMEM),
        compiler_params=SMALL,
    )(onset_steps[0], weights, slip_rate[0])

    code_rows = -(-capacity * points // CODE_ROWS) * CODE_ROWS
    outgoing = pl.pallas_call(
        functools.partial(contract_kernel, slots=capacity, points=points, strains=strains),
        name="contract",
        out_shape=jax.ShapeDtypeStruct((devices, capacity * points * rows + code_rows, LANES), jnp.int16),
        in_specs=[SMEM, VMEM],
        out_specs=VMEM,
        compiler_params=SMALL,
    )(asked, tensors)
    incoming = lax.all_to_all(outgoing, "pts", split_axis=0, concat_axis=0, tiled=True)

    result = pl.pallas_call(
        functools.partial(synth_kernel, listed=listed, points=points, slots=capacity),
        name="synthesize",
        out_shape=jax.ShapeDtypeStruct((variations, rows, LANES), F32),
        in_specs=[SMEM, VMEM, VMEM, VMEM, VMEM],
        out_specs=VMEM,
        compiler_params=LARGE,
        scratch_shapes=[
            pltpu.VMEM((q * rows, LANES), F32),
            pltpu.VMEM((comps, 2 * FINE * q, blocks * LANES), BF16),
            pltpu.VMEM((comps, coarse_rows, blocks * LANES), F32),
            pltpu.VMEM((variations * (rows + FINE), LANES), F32),
        ],
    )(slot_of, incoming, *prepared)
    result = result.reshape(variations, blocks, comps, LANES).transpose(0, 2, 1, 3)
    return result.reshape(1, variations, comps, length)


def solution(mesh):
    in_specs = (
        P(("site", "pts"), None, None, None, None),
        P(("site", "pts"), None),
        P(("site", "pts")),
        P(("site", "pts"), None, None),
        P(("site", "pts"), None, None),
        P(("site", "pts"), None),
        P(("site", "pts"), None, None),
    )
    out_specs = P(("site", "pts"), None, None, None)
    return jax.shard_map(local, mesh=mesh, in_specs=in_specs, out_specs=out_specs, check_vma=False)
```

```python
import functools

import jax
import jax.numpy as jnp
from jax import lax
from jax.experimental import pallas as pl
from jax.experimental.pallas import tpu as pltpu
from jax.sharding import PartitionSpec as P

MAXON = 256
FINE = 8
LANES = 128
F32 = jnp.float32
BF16 = jnp.bfloat16


def split(x):
    hi = x.astype(BF16)
    return hi, (x - hi.astype(F32)).astype(BF16)


def dot(a, b):
    return jnp.dot(a, b, preferred_element_type=F32)


def request_kernel(lists_ref, mech_ref, request_ref, slot_ref, *, held, capacity):
    devices = request_ref.shape[0]
    listed = lists_ref.shape[1]
    entries = lists_ref[...].astype(F32)
    holder = jnp.floor((entries + 0.5) * (1.0 / held))
    inside = entries - holder * held
    row = lax.broadcasted_iota(jnp.int32, (listed, listed), 0)
    col = lax.broadcasted_iota(jnp.int32, (listed, listed), 1)
    across = jnp.broadcast_to(holder, (listed, listed))
    down = jnp.sum(jnp.where(row == col, across, 0.0), axis=1, keepdims=True)
    same = jnp.where((down == across) & (row < col), 1.0, 0.0)
    rank = jnp.sum(same, axis=0, keepdims=True)
    slot_ref[...] = (holder * capacity + rank).astype(jnp.int32)
    request_ref[:, capacity:] = jnp.broadcast_to(mech_ref[...], (devices, mech_ref.shape[1]))
    device = lax.broadcasted_iota(jnp.int32, (devices, listed), 0).astype(F32)
    for j in range(capacity):
        hit = (device == holder) & (rank == j)
        request_ref[:, j:j + 1] = jnp.sum(jnp.where(hit, inside, 0.0), axis=1, keepdims=True)


CODE_STEPS = 256.0
CODE_BIAS = 100.0
VALUE_TOP = 32767.0
CODE_ROWS = 8


def encode(x):
    top = jnp.max(jnp.max(jnp.abs(x), axis=0, keepdims=True), axis=1, keepdims=True)
    code = jnp.ceil((jnp.log2(jnp.maximum(top, 1e-30)) + CODE_BIAS) * CODE_STEPS)
    code = jnp.broadcast_to(code, (1, LANES))
    scale = jnp.exp2(15.0 - (code * (1.0 / CODE_STEPS) - CODE_BIAS))
    value = jnp.clip(jnp.floor(x * scale + 0.5), -VALUE_TOP, VALUE_TOP)
    return value.astype(jnp.int32).astype(jnp.int16), code


def decode(y, codes, entry):
    place = lax.broadcasted_iota(jnp.int32, codes.shape, 0)
    code = jnp.sum(jnp.where(place == entry, codes, 0.0), axis=0, keepdims=True)
    scale = jnp.exp2((code * (1.0 / CODE_STEPS) - CODE_BIAS) - 15.0)
    return y.astype(jnp.int32).astype(F32) * scale


def contract_kernel(asked_ref, tensors_ref, out_ref, *, slots, points, strains):
    rows = tensors_ref.shape[3]
    code_rows = out_ref.shape[1] - slots * points * rows

    def one_source(source, carry):
        factors = [asked_ref[source, slots + s] for s in range(strains)]
        place = lax.broadcasted_iota(jnp.int32, (code_rows, LANES), 0)
        codes = jnp.zeros((code_rows, LANES), F32)
        for j in range(slots):
            block = asked_ref[source, j].astype(jnp.int32)
            for p in range(points):
                total = factors[0] * tensors_ref[block, p, 0].astype(F32)
                for s in range(1, strains):
                    total = total + factors[s] * tensors_ref[block, p, s].astype(F32)
                entry = j * points + p
                value, code = encode(total)
                out_ref[source, pl.ds(entry * rows, rows), :] = value
                codes = jnp.where(place == entry, code, codes)
        out_ref[source, pl.ds(slots * points * rows, code_rows), :] = codes.astype(jnp.int32).astype(jnp.int16)
        return carry

    lax.fori_loop(0, out_ref.shape[0], one_source, 0, unroll=2)


def prepare_kernel(onset_ref, weight_ref, a_ref):
    variations, points = onset_ref.shape
    width = FINE * points
    onsets = onset_ref[...]
    weights = weight_ref[...]
    w_hi = weights.astype(BF16).astype(F32)
    w_lo = weights - w_hi
    for coarse in range(MAXON // FINE):
        for fine in range(FINE):
            hit = onsets == coarse * FINE + fine
            rows = pl.ds(coarse * variations, variations)
            near = jnp.where(hit, w_hi, 0.0).astype(BF16)
            a_ref[rows, pl.ds(fine * points, points)] = near
            a_ref[rows, pl.ds(width + fine * points, points)] = near
            a_ref[rows, pl.ds(2 * width + fine * points, points)] = jnp.where(hit, w_lo, 0.0).astype(BF16)


def synth_kernel(row_ref, got_ref, a_ref, rate_ref, out_ref,
                 base_ref, x_ref, acc_ref, motion_ref, *, listed, points, slots):
    variations, rows = out_ref.shape[:2]
    q = listed * points
    comps = 2
    blocks = rows // comps

    code_rows = got_ref.shape[1] - slots * points * rows

    def place(k, carry):
        slot = row_ref[0, k]
        source = slot // slots
        first = (slot % slots) * points
        codes = got_ref[source, pl.ds(slots * points * rows, code_rows), :].astype(jnp.int32).astype(F32)
        for p in range(points):
            value = got_ref[source, pl.ds(pl.multiple_of((first + p) * rows, rows), rows), :]
            base_ref[pl.ds(pl.multiple_of((k * points + p) * rows, rows), rows), :] = decode(value, codes, first + p)
        return carry

    lax.fori_loop(0, listed, place, 0, unroll=4)
    lane = lax.broadcasted_iota(jnp.int32, (q, LANES), 1)
    for c in range(comps):
        before = [jnp.zeros((q, LANES), F32)] * FINE
        for block in range(blocks):
            r = block * comps + c
            here = base_ref[pl.ds(r, q, stride=rows), :]
            at = pl.ds(block * LANES, LANES)
            for fine in range(FINE):
                turned = pltpu.roll(here, fine, 1) if fine else here
                value = jnp.where(lane >= fine, turned, before[fine]) if fine else here
                hi, lo = split(value)
                x_ref[c, pl.ds(fine * q, q), at] = hi
                x_ref[c, pl.ds((FINE + fine) * q, q), at] = lo
                before[fine] = turned
        both = 2 * FINE * q
        acc_ref[c] = dot(a_ref[:, :both], x_ref[c]) + dot(a_ref[:, both:], x_ref[c, :FINE * q])
    lane = lax.broadcasted_iota(jnp.int32, (variations, LANES), 1)
    zero = jnp.zeros((variations, LANES), F32)
    half = LANES // FINE
    far_count = MAXON // LANES
    pad = motion_ref.shape[0] // variations
    motion_ref[...] = jnp.zeros(motion_ref.shape, F32)
    for c in range(comps):
        before = [zero] * half
        for block in range(blocks):
            total = zero
            for coarse in range(half):
                value = zero
                for far in range(far_count):
                    if block - far < 0:
                        continue
                    at = pl.ds((block - far) * LANES, LANES)
                    value = value + acc_ref[c, pl.ds((far * half + coarse) * variations, variations), at]
                turned = pltpu.roll(value, coarse * FINE, 1) if coarse else value
                total = total + (jnp.where(lane >= coarse * FINE, turned, before[coarse]) if coarse else turned)
                before[coarse] = turned
            motion_ref[pl.ds(FINE + block * comps + c, variations, stride=pad), :] = total
    taps = rate_ref.shape[1]
    row = lax.broadcasted_iota(jnp.int32, (taps, taps), 0)
    col = lax.broadcasted_iota(jnp.int32, (taps, taps), 1)
    for v in range(variations):
        rates = jnp.broadcast_to(rate_ref[pl.ds(v, 1), :], (taps, taps))
        turned = pltpu.roll(rates, 0, 1, stride=1, stride_axis=0)
        spread = [jnp.where(col >= row, turned, 0.0), jnp.where(col < row, turned, 0.0)]
        t_hi, t_lo = split(jnp.concatenate(spread, axis=0))
        here = motion_ref[pl.ds(v * pad + FINE, rows), :]
        earlier = motion_ref[pl.ds(v * pad + FINE - comps, rows), :]
        h_hi, h_lo = split(jnp.concatenate([here, earlier], axis=1))
        out_ref[v] = dot(h_hi, t_hi) + (dot(h_lo, t_hi) + dot(h_hi, t_lo))


SMALL = pltpu.CompilerParams(vmem_limit_bytes=8 << 20)
LARGE = pltpu.CompilerParams(vmem_limit_bytes=20 << 20)
VMEM = pl.BlockSpec(memory_space=pltpu.VMEM)
SMEM = pl.BlockSpec(memory_space=pltpu.SMEM)


def local(green_tensors, block_lists, block_count, onset_steps, slip_amount, mechanism, slip_rate):
    held, points, strains, comps, length = green_tensors.shape
    ruptures, listed = block_lists.shape
    variations = onset_steps.shape[1]
    devices = lax.axis_size("pts")
    capacity = max(1, ruptures * listed // devices)
    blocks = length // LANES
    rows = blocks * comps
    q = listed * points

    tensors = green_tensors.reshape(held, points, strains, comps, blocks, LANES)
    tensors = tensors.transpose(0, 1, 2, 4, 3, 5).reshape(held, points, strains, rows, LANES)

    request, slot_of = pl.pallas_call(
        functools.partial(request_kernel, held=held, capacity=capacity),
        name="request",
        out_shape=(
            jax.ShapeDtypeStruct((devices, capacity + strains), F32),
            jax.ShapeDtypeStruct((ruptures, listed), jnp.int32),
        ),
        compiler_params=SMALL,
    )(block_lists, mechanism)
    asked = lax.all_to_all(request, "pts", split_axis=0, concat_axis=0, tiled=True)

    kept = (jnp.arange(q, dtype=jnp.int32) // points) < block_count[0]
    weights = jnp.where(kept[None, :], slip_amount[0], 0.0)
    coarse_rows = MAXON // FINE * variations
    prepared = pl.pallas_call(
        prepare_kernel,
        name="prepare",
        out_shape=jax.ShapeDtypeStruct((coarse_rows, 3 * FINE * q), BF16),
        in_specs=[VMEM, VMEM],
        out_specs=VMEM,
        compiler_params=SMALL,
    )(onset_steps[0], weights)

    code_rows = -(-capacity * points // CODE_ROWS) * CODE_ROWS
    outgoing = pl.pallas_call(
        functools.partial(contract_kernel, slots=capacity, points=points, strains=strains),
        name="contract",
        out_shape=jax.ShapeDtypeStruct((devices, capacity * points * rows + code_rows, LANES), jnp.int16),
        in_specs=[SMEM, VMEM],
        out_specs=VMEM,
        compiler_params=SMALL,
    )(asked, tensors)
    incoming = lax.all_to_all(outgoing, "pts", split_axis=0, concat_axis=0, tiled=True)

    result = pl.pallas_call(
        functools.partial(synth_kernel, listed=listed, points=points, slots=capacity),
        name="synthesize",
        out_shape=jax.ShapeDtypeStruct((variations, rows, LANES), F32),
        in_specs=[SMEM, VMEM, VMEM, VMEM],
        out_specs=VMEM,
        compiler_params=LARGE,
        scratch_shapes=[
            pltpu.VMEM((q * rows, LANES), F32),
            pltpu.VMEM((comps, 2 * FINE * q, blocks * LANES), BF16),
            pltpu.VMEM((comps, coarse_rows, blocks * LANES), F32),
            pltpu.VMEM((variations * (rows + FINE), LANES), F32),
        ],
    )(slot_of, incoming, prepared, slip_rate[0])
    result = result.reshape(variations, blocks, comps, LANES).transpose(0, 2, 1, 3)
    return result.reshape(1, variations, comps, length)


def solution(mesh):
    in_specs = (
        P(("site", "pts"), None, None, None, None),
        P(("site", "pts"), None),
        P(("site", "pts")),
        P(("site", "pts"), None, None),
        P(("site", "pts"), None, None),
        P(("site", "pts"), None),
        P(("site", "pts"), None, None),
    )
    out_specs = P(("site", "pts"), None, None, None)
    return jax.shard_map(local, mesh=mesh, in_specs=in_specs, out_specs=out_specs, check_vma=False)
```
